768 devices in a mesh: dp: 128 (over x, y, z_lo), tensor: 6 (over z_hi, core).
Axes of the slice: x: 4, y: 8, z: 12 (z_hi: 3, z_lo: 4; z = z_hi * 4 + z_lo), core: 2. Of those that a mesh axis runs over, the one named last changes fastest.
Arguments:
- latent_raw: bfloat16 [24576, 512], P('dp'), may hold values from -24 to 24
- norm_gain: float32 [512], replicated, may hold values from 0.5 to 1.5
- up_weight: bfloat16 [512, 24576], P(None, 'tensor'), may hold values from -0.25 to 0.25
- grad_kv: bfloat16 [24576, 24576], P('dp', 'tensor'), may hold values from -3 to 3
Outputs:
- latent_grad: bfloat16 [24576, 512], P('dp')
- gain_grad: float32 [512], replicated
- weight_grad: float32 [512, 24576], P('dp', 'tensor')
The draws below stay inside these ranges and needn't reach their ends.
All inputs are finite; a program needn't handle non-finite values.
Results may differ from the reference program's by a relative error of at most 0.0029.
Values may be sent and summed in bfloat16 or wider, within the bound.
A program may use at most 64 MiB of HBM per device.

```python
import jax
import jax.numpy as jnp
from jax import lax

KVL = 512
HEAD_DIM = 128
HEADS = 96
TOKENS = 24576


def strengthened(drawn, rng, source, target, blocks, factor):
    owner, partner = [(jnp.arange(drawn.shape[position]) // (drawn.shape[position] // blocks)).reshape([-1 if axis == position else 1 for axis in range(drawn.ndim)]) for position in (source, target)]
    chosen = jax.random.permutation(rng, blocks)[partner]
    strong = (owner == chosen) | (owner == (partner + blocks // 2) % blocks)
    return jnp.where(strong, factor * drawn, drawn)


def steps_of(rng, extent, shards, least, high):
    level = 1.0
    for position, parts in shards:
        draws = jax.random.uniform(jax.random.fold_in(jax.random.fold_in(rng, 6), position), (parts,), jnp.float32, least / len(shards), high / len(shards))
        level = level * jnp.repeat(jnp.exp(draws), extent[position] // parts).reshape((-1,) + (1,) * (len(extent) - 1 - position))
    return level


def noise(stream_key, shape, scale, bound, split=(), held_as=jnp.bfloat16):
    factor_of = steps_of(stream_key, shape, split, -0.22, 0.18) if split else 1.0
    entries = jax.random.normal(stream_key, shape, jnp.float32) * scale * factor_of
    return jnp.minimum(jnp.maximum(entries, -bound), bound).astype(held_as)


def bell_draw_with(stream_key, extent, spread, most, shards, heavy, dtype=jnp.bfloat16):
    array = spread * jax.random.normal(stream_key, extent, jnp.float32)
    if shards:
        array = array * steps_of(stream_key, extent, shards, -0.22, 0.18)
    return jnp.clip(strengthened(array, jax.random.fold_in(stream_key, 3), *heavy), -most, most).astype(dtype)


def setup_inputs(seed: int = 0) -> dict:
    arg_keys = jax.random.split(jax.random.key(seed), 5)
    return {
        "latent_raw": bell_draw_with(arg_keys[0], (TOKENS, KVL), 1.0, 24.0, ((0, 128),), (0, 1, 128, 5.5)),
        "norm_gain": jnp.clip(1.0 + 0.1 * jax.random.normal(arg_keys[1], (KVL,), jnp.float32), 0.5, 1.5),
        "up_weight": noise(arg_keys[2], (KVL, HEADS * 2 * HEAD_DIM), KVL ** -0.5, 0.25, ((1, 6),)),
        "grad_kv": noise(arg_keys[3], (TOKENS, HEADS * 2 * HEAD_DIM), 0.5, 3.0, ((0, 128), (1, 6))),
    }


epsilon = 1e-06

def reference(latent_raw, norm_gain, up_weight, grad_kv):
    latent_full = latent_raw.astype(jnp.float32)
    inverse = lax.rsqrt(lax.optimization_barrier(jnp.mean(latent_full * latent_full, axis=-1, keepdims=True)) + epsilon)
    scaled_rows = latent_full * inverse
    normed = (scaled_rows * norm_gain).astype(jnp.bfloat16)
    factor = float(TOKENS) ** (-0.5)
    grad_norm = lax.dot_general(grad_kv, up_weight, (((1,), (1,)), ((), ())), preferred_element_type=jnp.float32)
    gain_grad = lax.optimization_barrier(jnp.sum(grad_norm * scaled_rows, axis=0)) * factor
    upstream = grad_norm * norm_gain
    centred = upstream - scaled_rows * lax.optimization_barrier(jnp.mean(upstream * scaled_rows, axis=-1, keepdims=True))
    latent_grad = (inverse * centred).astype(jnp.bfloat16)
    weight_grad = lax.dot_general(normed, grad_kv, (((0,), (0,)), ((), ())), preferred_element_type=jnp.float32) * factor
    return (latent_grad, gain_grad, weight_grad)
```

```python
import functools

import jax
import jax.numpy as jnp
from jax import lax
from jax.experimental import pallas as pl
from jax.experimental.pallas import tpu as pltpu
from jax.sharding import Mesh
from jax.sharding import PartitionSpec as P

X, Y, Z, H, C = AXES = ("dp_0", "dp_1", "dp_2", "tensor_0", "tensor_1")
DP = (X, Y, Z)
TENSOR = (H, C)
NX, NY, NZ, NH, NC = 4, 8, 4, 3, 2
NT = NH * NC
SIZE = dict(zip(AXES, (NX, NY, NZ, NH, NC)))
MESH = pl.DeviceIdType.MESH

KVL = 512
COLS = 4096
ROWS = 192
BLOCK = COLS // NX
PART = ROWS // NT
OWN = KVL // (NX * NY * NZ)
STRIP = OWN * NZ
epsilon = 1e-06

CHUNKS = ((0, 256), (256, 256), (512, 256), (768, 256))
BATCHES = ((0, 768), (768, 256))
LAST_OF_BATCH = {2: 0, 3: 1}

X_OFFSETS = (1, 3, 2)
Y_OFFSETS = (1, 7, 2, 6, 3, 5, 4)
XZ_OFFSETS = tuple((i, j) for i in range(NX) for j in range(NZ) if (i, j) != (0, 0))
T_OFFSETS = tuple((i, j) for i in range(NH) for j in range(NC) if (i, j) != (0, 0))


def shifted(axis, offset):
    return lax.rem(lax.axis_index(axis) + (offset % SIZE[axis]), SIZE[axis])


def at(**offsets):
    return {axis: shifted(axis, offset) for axis, offset in offsets.items() if offset % SIZE[axis]}


def normalize(latent):
    full = latent.astype(jnp.float32)
    inverse = lax.rsqrt(jnp.mean(full * full, axis=-1, keepdims=True) + epsilon)
    return full * inverse, inverse


def kernel(
    factor,
    latent_hbm, gain_ref, up_hbm, grad_hbm,
    latent_out, gain_out, weight_out,
    latent, up, grad, normed, tokens, full, wsend, ybuf, esend, ebuf, tsend, tbuf, lbuf,
    g1, g2, g3,
    local_sem, xs, xr, ys, yr, es, er, ts, tr, ls, lr, gs, gr,
):
    x, y, z = (lax.axis_index(a) for a in DP)
    t = lax.axis_index(H) * NC + lax.axis_index(C)
    sends = []

    def send(src, dst, send_sem, recv_sem, device):
        copy = pltpu.make_async_remote_copy(
            src_ref=src, dst_ref=dst, send_sem=send_sem, recv_sem=recv_sem,
            device_id=device, device_id_type=MESH,
        )
        copy.start()
        sends.append(copy)
        return copy

    loads = [
        pltpu.make_async_copy(latent_hbm, latent, local_sem.at[0]),
        pltpu.make_async_copy(grad_hbm, grad, local_sem.at[1]),
        pltpu.make_async_copy(
            grad_hbm.at[:, pl.ds(pl.multiple_of(x * BLOCK, BLOCK), BLOCK)],
            tokens.at[pl.ds(0, ROWS), :], local_sem.at[2],
        ),
        pltpu.make_async_copy(up_hbm, up, local_sem.at[3]),
    ]
    for load in loads:
        load.start()

    barrier = pltpu.get_barrier_semaphore()
    devices = [at(**{X: i, Z: j}) for i, j in XZ_OFFSETS]
    devices += [at(**{Y: i}) for i in Y_OFFSETS]
    devices += [at(**{H: i, C: j}) for i, j in T_OFFSETS]
    for device in devices:
        pl.semaphore_signal(barrier, inc=1, device_id=device, device_id_type=MESH)

    loads[0].wait()
    scaled, _ = normalize(latent[...])
    normed[pl.ds(0, ROWS), :] = (scaled * gain_ref[...]).astype(jnp.bfloat16)
    loads[1].wait()
    pl.semaphore_wait(barrier, len(devices))

    nsends = {}
    for n, i in enumerate(X_OFFSETS):
        nsends[i] = send(
            normed.at[pl.ds(0, ROWS), :], normed.at[pl.ds(ROWS * i, ROWS), :],
            xs.at[n, len(CHUNKS)], xr.at[n, len(CHUNKS)], at(**{X: i}),
        )
    xsends = {}
    for k, (start, width) in enumerate(CHUNKS):
        for n, i in enumerate(X_OFFSETS):
            column = pl.multiple_of(shifted(X, i) * BLOCK + start, 128)
            xsends[k, i] = send(
                grad.at[:, pl.ds(column, width)],
                tokens.at[pl.ds(ROWS * i, ROWS), pl.ds(start, width)],
                xs.at[n, k], xr.at[n, k], at(**{X: i}),
            )

    loads[3].wait()
    tsend[...] = lax.dot_general(
        grad[...], up[...], (((1,), (1,)), ((), ())), preferred_element_type=jnp.float32
    )
    tsends = []
    for n, (i, j) in enumerate(T_OFFSETS):
        other = shifted(H, i) * NC + shifted(C, j)
        tsends.append(send(
            tsend.at[pl.ds(pl.multiple_of(other * PART, PART), PART), :], tbuf.at[n],
            ts.at[n], tr.at[n], at(**{H: i, C: j}),
        ))
    loads[2].wait()

    def weight_chunk(k):
        start, width = CHUNKS[k]
        if k == 0:
            for i in X_OFFSETS:
                nsends[i].wait_recv()
        for i in X_OFFSETS:
            xsends[k, i].wait_recv()
        full[:, start : start + width] = lax.dot_general(
            normed[...], tokens[:, start : start + width], (((0,), (0,)), ((), ())),
            preferred_element_type=jnp.float32,
        )
        for q in range(NY):
            for p in range(NX):
                wsend[q, STRIP * p : STRIP * (p + 1), start : start + width] = full[
                    128 * p + STRIP * q : 128 * p + STRIP * (q + 1), start : start + width
                ].astype(jnp.bfloat16)
        copies = []
        for n, i in enumerate(Y_OFFSETS):
            copies.append(send(
                wsend.at[shifted(Y, i), :, pl.ds(start, width)],
                ybuf.at[n, :, pl.ds(start, width)],
                ys.at[n, k], yr.at[n, k], at(**{Y: i}),
            ))
        return copies

    def sum_chunk(k, copies):
        start, width = CHUNKS[k]
        for copy in copies:
            copy.wait_recv()
        for p in range(NX):
            row = pl.multiple_of(128 * p + STRIP * y, STRIP)
            total = full[pl.ds(row, STRIP), start : start + width]
            for n in range(NY - 1):
                total = total + ybuf[
                    n, STRIP * p : STRIP * (p + 1), start : start + width
                ].astype(jnp.float32)
            for q in range(NZ):
                esend[NZ * p + q, :, start : start + width] = total[OWN * q : OWN * (q + 1)]

    def exchange(b):
        start, width = BATCHES[b]
        copies = []
        for n, (i, j) in enumerate(XZ_OFFSETS):
            copies.append(send(
                esend.at[shifted(X, i) * NZ + shifted(Z, j), :, pl.ds(start, width)],
                ebuf.at[n, :, pl.ds(start, width)],
                es.at[n, b], er.at[n, b], at(**{X: i, Z: j}),
            ))
        return copies

    def latent_step():
        for copy in tsends:
            copy.wait_recv()
        own = pl.ds(pl.multiple_of(t * PART, PART), PART)
        grad_norm = tsend[own, :]
        for n in range(NT - 1):
            grad_norm = grad_norm + tbuf[n]
        scaled, inverse = normalize(latent[own, :])
        g1[t] = jnp.sum(grad_norm * scaled, axis=0, keepdims=True)
        upstream = grad_norm * gain_ref[...]
        centred = upstream - scaled * jnp.mean(upstream * scaled, axis=-1, keepdims=True)
        lbuf[own, :] = (inverse * centred).astype(jnp.bfloat16)
        copies = []
        for n, (i, j) in enumerate(T_OFFSETS):
            copies.append(send(
                g1.at[t], g1.at[t], gs.at[n], gr.at[n], at(**{H: i, C: j})
            ))
        lcopies = []
        for n, (i, j) in enumerate(T_OFFSETS):
            lcopies.append(send(
                lbuf.at[own, :], lbuf.at[own, :], ls.at[n], lr.at[n], at(**{H: i, C: j})
            ))
        return copies, lcopies

    def gain_step(copies, source, target, slot, offsets, first):
        for copy in copies:
            copy.wait_recv()
        total = source[0]
        for n in range(1, source.shape[0]):
            total = total + source[n]
        target[slot] = total
        copies = []
        for n, offset in enumerate(offsets):
            copies.append(send(
                target.at[slot], target.at[slot], gs.at[first + n], gr.at[first + n], at(**offset)
            ))
        return copies

    last = len(CHUNKS) - 1
    received = []
    pending = None
    for k in range(len(CHUNKS)):
        copies = weight_chunk(k)
        if pending is not None:
            sum_chunk(k - 1, pending)
            if k - 1 in LAST_OF_BATCH:
                received += exchange(LAST_OF_BATCH[k - 1])
        pending = copies
        if k == 1:
            gcopies, lcopies = latent_step()
        if k == last:
            gcopies = gain_step(
                gcopies, g1, g2, x * NZ + z, [{X: i, Z: j} for i, j in XZ_OFFSETS], NT - 1
            )
    sum_chunk(last, pending)
    received += exchange(LAST_OF_BATCH[last])
    gcopies = gain_step(
        gcopies, g2, g3, y, [{Y: i} for i in Y_OFFSETS], NT - 1 + NX * NZ - 1
    )
    for copy in lcopies:
        copy.wait_recv()
    latent_out[...] = lbuf[...]
    for copy in received:
        copy.wait_recv()
    for i in range(NX):
        total = None
        for j in range(NZ):
            if (i, j) == (0, 0):
                term = esend[x * NZ + z]
            else:
                term = ebuf[XZ_OFFSETS.index((i, j))]
            total = term if total is None else total + term
        column = pl.multiple_of(shifted(X, -i) * BLOCK, BLOCK)
        weight_out[:, pl.ds(column, BLOCK)] = total * factor
    for copy in gcopies:
        copy.wait_recv()
    total = g3[0]
    for n in range(1, NY):
        total = total + g3[n]
    gain_out[...] = total * factor
    for copy in sends:
        copy.wait_send()


def per_device(latent_raw, norm_gain, up_weight, grad_kv):
    factor = float(latent_raw.shape[0] * NX * NY * NZ) ** (-0.5)
    vmem = pl.BlockSpec(memory_space=pltpu.VMEM)
    hbm = pl.BlockSpec(memory_space=pl.ANY)
    dma = pltpu.SemaphoreType.DMA
    gains = NT - 1 + NX * NZ - 1 + NY - 1
    latent_grad, gain_grad, weight_grad = pl.pallas_call(
        functools.partial(kernel, factor),
        out_shape=(
            jax.ShapeDtypeStruct((ROWS, KVL), jnp.bfloat16),
            jax.ShapeDtypeStruct((1, KVL), jnp.float32),
            jax.ShapeDtypeStruct((OWN, COLS), jnp.float32),
        ),
        in_specs=[hbm, vmem, hbm, hbm],
        out_specs=(vmem, vmem, vmem),
        scratch_shapes=[
            pltpu.VMEM((ROWS, KVL), jnp.bfloat16),
            pltpu.VMEM((KVL, COLS), jnp.bfloat16),
            pltpu.VMEM((ROWS, COLS), jnp.bfloat16),
            pltpu.VMEM((NX * ROWS, KVL), jnp.bfloat16),
            pltpu.VMEM((NX * ROWS, BLOCK), jnp.bfloat16),
            pltpu.VMEM((KVL, BLOCK), jnp.float32),
            pltpu.VMEM((NY, STRIP * NX, BLOCK), jnp.bfloat16),
            pltpu.VMEM((NY - 1, STRIP * NX, BLOCK), jnp.bfloat16),
            pltpu.VMEM((NX * NZ, OWN, BLOCK), jnp.float32),
            pltpu.VMEM((NX * NZ - 1, OWN, BLOCK), jnp.float32),
            pltpu.VMEM((ROWS, KVL), jnp.float32),
            pltpu.VMEM((NT - 1, PART, KVL), jnp.float32),
            pltpu.VMEM((ROWS, KVL), jnp.bfloat16),
            pltpu.VMEM((NT, 1, KVL), jnp.float32),
            pltpu.VMEM((NX * NZ, 1, KVL), jnp.float32),
            pltpu.VMEM((NY, 1, KVL), jnp.float32),
            dma((4,)),
            dma((NX - 1, len(CHUNKS) + 1)),
            dma((NX - 1, len(CHUNKS) + 1)),
            dma((NY - 1, len(CHUNKS))),
            dma((NY - 1, len(CHUNKS))),
            dma((NX * NZ - 1, len(BATCHES))),
            dma((NX * NZ - 1, len(BATCHES))),
            dma((NT - 1,)),
            dma((NT - 1,)),
            dma((NT - 1,)),
            dma((NT - 1,)),
            dma((gains,)),
            dma((gains,)),
        ],
        compiler_params=pltpu.CompilerParams(collective_id=0, has_side_effects=True),
        name="norm_up_backward",
    )(latent_raw, norm_gain.reshape(1, KVL), up_weight, grad_kv)
    return latent_grad, gain_grad.reshape(KVL), weight_grad


def solution(mesh):
    split = Mesh(mesh.devices.reshape(NX, NY, NZ, NH, NC), AXES)
    in_specs = (P(DP, None), P(), P(None, TENSOR), P(DP, TENSOR))
    out_specs = (P(DP, None), P(), P(DP, TENSOR))
    return jax.shard_map(
        per_device, mesh=split, in_specs=in_specs, out_specs=out_specs, check_vma=False
    )
```

```python
import functools

import jax
import jax.numpy as jnp
from jax import lax
from jax.experimental import pallas as pl
from jax.experimental.pallas import tpu as pltpu
from jax.sharding import Mesh
from jax.sharding import PartitionSpec as P

X, Y, Z, H, C = AXES = ("dp_0", "dp_1", "dp_2", "tensor_0", "tensor_1")
DP = (X, Y, Z)
TENSOR = (H, C)
NX, NY, NZ, NH, NC = 4, 8, 4, 3, 2
NT = NH * NC
SIZE = dict(zip(AXES, (NX, NY, NZ, NH, NC)))
MESH = pl.DeviceIdType.MESH

KVL = 512
COLS = 4096
ROWS = 192
BLOCK = COLS // NX
PART = ROWS // NT
OWN = KVL // (NX * NY * NZ)
STRIP = OWN * NZ
epsilon = 1e-06

CHUNKS = ((0, 256), (256, 256), (512, 256), (768, 128), (896, 128))
BATCHES = ((0, 512), (512, 384), (896, 128))
BATCH_AFTER = {1: 0, 3: 1, 4: 2}
SCHEDULE = "W0 W1 R0 G1 W2 R1 S0 W3 G2 W4 R2 S1 R3 R4 G3 S2 S3 S4"
HALF = ROWS // NC
PIECE = OWN * NZ * NX

X_OFFSETS = (1, 3, 2)
Y_OFFSETS = (1, 7, 2, 6, 3, 5, 4)
XZ_OFFSETS = tuple((i, j) for i in range(NX) for j in range(NZ) if (i, j) != (0, 0))
T_OFFSETS = tuple((i, j) for i in range(NH) for j in range(NC) if (i, j) != (0, 0))


def shifted(axis, offset):
    return lax.rem(lax.axis_index(axis) + (offset % SIZE[axis]), SIZE[axis])


def at(**offsets):
    return {axis: shifted(axis, offset) for axis, offset in offsets.items() if offset % SIZE[axis]}


def normalize(latent):
    full = latent.astype(jnp.float32)
    inverse = lax.rsqrt(jnp.mean(full * full, axis=-1, keepdims=True) + epsilon)
    return full * inverse, inverse


def kernel(
    factor,
    latent_hbm, gain_hbm, up_hbm, grad_hbm,
    latent_out, gain_out, weight_out,
    latent, gain, up, grad, normed, tokens, full, wsend, direct, far, farther, rsend, relayed,
    esend, ebuf, tsend, tbuf, g1, g2, g3,
    local_sem, ns, nr, fs, fr, xs, xr, ys, yr, es, er, ts, tr, ls, lr, gs, gr,
):
    x, y, z = (lax.axis_index(a) for a in DP)
    core = lax.axis_index(C)
    t = lax.axis_index(H) * NC + core
    sends = []

    def send(src, dst, send_sem, recv_sem, device):
        copy = pltpu.make_async_remote_copy(
            src_ref=src, dst_ref=dst, send_sem=send_sem, recv_sem=recv_sem,
            device_id=device, device_id_type=MESH,
        )
        copy.start()
        sends.append(copy)
        return copy

    loads = [
        pltpu.make_async_copy(latent_hbm, latent, local_sem.at[0]),
        pltpu.make_async_copy(gain_hbm, gain, local_sem.at[1]),
        pltpu.make_async_copy(grad_hbm, grad, local_sem.at[2]),
        pltpu.make_async_copy(
            grad_hbm.at[:, pl.ds(pl.multiple_of(x * BLOCK, BLOCK), BLOCK)],
            tokens.at[pl.ds(0, ROWS), :], local_sem.at[3],
        ),
        pltpu.make_async_copy(up_hbm, up, local_sem.at[4]),
    ]
    for load in loads:
        load.start()

    barrier = pltpu.get_barrier_semaphore()
    devices = [at(**{H: i, C: j}) for i, j in T_OFFSETS]
    devices += [at(**{X: i, Z: j}) for i, j in XZ_OFFSETS]
    devices += [at(**{Y: i}) for i in Y_OFFSETS]
    for device in devices:
        pl.semaphore_signal(barrier, inc=1, device_id=device, device_id_type=MESH)

    loads[0].wait()
    loads[1].wait()
    scaled, _ = normalize(latent[...])
    normed[pl.ds(0, ROWS), :] = (scaled * gain[...]).astype(jnp.bfloat16)
    pl.semaphore_wait(barrier, len(devices))

    def half(i):
        return pl.ds(pl.multiple_of(ROWS * i + HALF * core, HALF), HALF)

    halves = []
    for n, i in enumerate(X_OFFSETS):
        halves.append(send(
            normed.at[half(0), :], normed.at[half(i), :], ns.at[n], nr.at[n], at(**{X: i})
        ))
    loads[2].wait()
    xsends = {}
    for k, (start, width) in enumerate(CHUNKS):
        for n, i in enumerate(X_OFFSETS):
            column = pl.multiple_of(shifted(X, i) * BLOCK + start, 128)
            xsends[k, i] = send(
                grad.at[:, pl.ds(column, width)],
                tokens.at[pl.ds(ROWS * i, ROWS), pl.ds(start, width)],
                xs.at[n, k], xr.at[n, k], at(**{X: i}),
            )

    loads[4].wait()
    tsend[...] = lax.dot_general(
        grad[...], up[...], (((1,), (1,)), ((), ())), preferred_element_type=jnp.float32
    )
    tsends = []
    for n, (i, j) in enumerate(T_OFFSETS):
        other = shifted(H, i) * NC + shifted(C, j)
        tsends.append(send(
            tsend.at[pl.ds(pl.multiple_of(other * PART, PART), PART), :], tbuf.at[n],
            ts.at[n], tr.at[n], at(**{H: i, C: j}),
        ))
    loads[3].wait()
    forwards = []
    for n, i in enumerate(X_OFFSETS):
        halves[n].wait_recv()
        forwards.append(send(
            normed.at[half(i), :], normed.at[half(i), :], fs.at[n], fr.at[n], at(**{C: 1})
        ))

    def rows_of(other, p):
        return pl.ds(pl.multiple_of(128 * p + STRIP * other, STRIP), STRIP)

    def weight_chunk(k):
        start, width = CHUNKS[k]
        columns = slice(start, start + width)
        if k == 0:
            for copy in forwards:
                copy.wait_recv()
        for i in X_OFFSETS:
            xsends[k, i].wait_recv()
        full[:, columns] = lax.dot_general(
            normed[...], tokens[:, columns], (((0,), (0,)), ((), ())),
            preferred_element_type=jnp.float32,
        )
        for slot, offset in enumerate((3, -3, 4, 1, -1)):
            for p in range(NX):
                wsend[slot, STRIP * p : STRIP * (p + 1), columns] = full[
                    rows_of(shifted(Y, offset), p), columns
                ].astype(jnp.bfloat16)
        window = pl.ds(start, width)
        into_relay, into_total = [], []
        for side, sign in enumerate((1, -1)):
            into_relay.append(send(
                wsend.at[side, :, window], far.at[side, :, window],
                ys.at[side, k], yr.at[side, k], at(**{Y: sign}),
            ))
        for side, sign in enumerate((1, -1)):
            into_relay.append(send(
                wsend.at[2, pl.ds(PIECE // 2 * side, PIECE // 2), window],
                farther.at[side, :, window],
                ys.at[2 + side, k], yr.at[2 + side, k], at(**{Y: 2 * sign}),
            ))
        for side, sign in enumerate((1, -1)):
            into_total.append(send(
                wsend.at[3 + side, :, window], direct.at[side, :, window],
                ys.at[4 + side, k], yr.at[4 + side, k], at(**{Y: sign}),
            ))
        return into_relay, into_total

    def relay_chunk(k, into_relay):
        start, width = CHUNKS[k]
        columns = slice(start, start + width)
        for copy in into_relay:
            copy.wait_recv()
        copies = []
        for side, sign in enumerate((1, -1)):
            for p in range(NX):
                part = slice(STRIP * p, STRIP * (p + 1))
                total = full[rows_of(shifted(Y, 2 * sign), p), columns]
                total = total + far[side, part, columns].astype(jnp.float32)
                if p // 2 == side:
                    start_row = STRIP * (p - 2 * side)
                    total = total + farther[
                        side, start_row : start_row + STRIP, columns
                    ].astype(jnp.float32)
                rsend[side, part, columns] = total.astype(jnp.bfloat16)
            window = pl.ds(start, width)
            copies.append(send(
                rsend.at[side, :, window], relayed.at[side, :, window],
                ys.at[6 + side, k], yr.at[6 + side, k], at(**{Y: 2 * sign}),
            ))
        return copies

    def sum_chunk(k, copies):
        start, width = CHUNKS[k]
        columns = slice(start, start + width)
        for copy in copies:
            copy.wait_recv()
        for p in range(NX):
            part = slice(STRIP * p, STRIP * (p + 1))
            total = full[rows_of(y, p), columns]
            for source in (direct, relayed):
                for side in range(2):
                    total = total + source[side, part, columns].astype(jnp.float32)
            for q in range(NZ):
                esend[NZ * p + q, :, columns] = total[OWN * q : OWN * (q + 1)]

    def exchange(b):
        start, width = BATCHES[b]
        copies = []
        for n, (i, j) in enumerate(XZ_OFFSETS):
            copies.append(send(
                esend.at[shifted(X, i) * NZ + shifted(Z, j), :, pl.ds(start, width)],
                ebuf.at[n, :, pl.ds(start, width)],
                es.at[n, b], er.at[n, b], at(**{X: i, Z: j}),
            ))
        return copies

    def latent_step():
        for copy in tsends:
            copy.wait_recv()
        own = pl.ds(pl.multiple_of(t * PART, PART), PART)
        grad_norm = tsend[own, :]
        for n in range(NT - 1):
            grad_norm = grad_norm + tbuf[n]
        scaled, inverse = normalize(latent[own, :])
        g1[t] = jnp.sum(grad_norm * scaled, axis=0, keepdims=True)
        upstream = grad_norm * gain[...]
        centred = upstream - scaled * jnp.mean(upstream * scaled, axis=-1, keepdims=True)
        latent_out[own, :] = (inverse * centred).astype(jnp.bfloat16)
        copies = []
        for n, (i, j) in enumerate(T_OFFSETS):
            copies.append(send(
                g1.at[t], g1.at[t], gs.at[n], gr.at[n], at(**{H: i, C: j})
            ))
        lcopies = []
        for n, (i, j) in enumerate(T_OFFSETS):
            lcopies.append(send(
                latent_out.at[own, :], latent_out.at[own, :], ls.at[n], lr.at[n],
                at(**{H: i, C: j}),
            ))
        return copies, lcopies

    def gain_step(copies, source, target, slot, offsets, first):
        for copy in copies:
            copy.wait_recv()
        total = source[0]
        for n in range(1, source.shape[0]):
            total = total + source[n]
        target[slot] = total
        copies = []
        for n, offset in enumerate(offsets):
            copies.append(send(
                target.at[slot], target.at[slot], gs.at[first + n], gr.at[first + n], at(**offset)
            ))
        return copies

    into_relay, into_total, received = {}, {}, []
    gcopies = lcopies = None
    for step in SCHEDULE.split():
        kind, k = step[0], int(step[1:])
        if kind == "W":
            into_relay[k], into_total[k] = weight_chunk(k)
        elif kind == "R":
            into_total[k] += relay_chunk(k, into_relay[k])
        elif kind == "S":
            sum_chunk(k, into_total[k])
            if k in BATCH_AFTER:
                received += exchange(BATCH_AFTER[k])
        elif kind == "G" and k == 1:
            gcopies, lcopies = latent_step()
        elif kind == "G" and k == 2:
            gcopies = gain_step(
                gcopies, g1, g2, x * NZ + z, [{X: i, Z: j} for i, j in XZ_OFFSETS], NT - 1
            )
        else:
            gcopies = gain_step(
                gcopies, g2, g3, y, [{Y: i} for i in Y_OFFSETS], NT - 1 + NX * NZ - 1
            )
    for copy in lcopies:
        copy.wait_recv()
    for copy in received:
        copy.wait_recv()
    for i in range(NX):
        total = None
        for j in range(NZ):
            if (i, j) == (0, 0):
                term = esend[x * NZ + z]
            else:
                term = ebuf[XZ_OFFSETS.index((i, j))]
            total = term if total is None else total + term
        column = pl.multiple_of(shifted(X, -i) * BLOCK, BLOCK)
        weight_out[:, pl.ds(column, BLOCK)] = total * factor
    for copy in gcopies:
        copy.wait_recv()
    total = g3[0]
    for n in range(1, NY):
        total = total + g3[n]
    gain_out[...] = total * factor
    for copy in sends:
        copy.wait_send()


def store(*refs):
    for source, target in zip(refs[:3], refs[3:]):
        target[...] = source[...]


def per_device(latent_raw, norm_gain, up_weight, grad_kv):
    factor = float(latent_raw.shape[0] * NX * NY * NZ) ** (-0.5)
    vmem = pl.BlockSpec(memory_space=pltpu.VMEM)
    hbm = pl.BlockSpec(memory_space=pl.ANY)
    dma = pltpu.SemaphoreType.DMA
    gains = NT - 1 + NX * NZ - 1 + NY - 1
    chunks = len(CHUNKS)
    shapes = (
        jax.ShapeDtypeStruct((ROWS, KVL), jnp.bfloat16),
        jax.ShapeDtypeStruct((1, KVL), jnp.float32),
        jax.ShapeDtypeStruct((OWN, COLS), jnp.float32),
    )
    results = pl.pallas_call(
        functools.partial(kernel, factor),
        out_shape=shapes,
        in_specs=[hbm, hbm, hbm, hbm],
        out_specs=(vmem, vmem, vmem),
        scratch_shapes=[
            pltpu.VMEM((ROWS, KVL), jnp.bfloat16),
            pltpu.VMEM((1, KVL), jnp.float32),
            pltpu.VMEM((KVL, COLS), jnp.bfloat16),
            pltpu.VMEM((ROWS, COLS), jnp.bfloat16),
            pltpu.VMEM((NX * ROWS, KVL), jnp.bfloat16),
            pltpu.VMEM((NX * ROWS, BLOCK), jnp.bfloat16),
            pltpu.VMEM((KVL, BLOCK), jnp.float32),
            pltpu.VMEM((5, PIECE, BLOCK), jnp.bfloat16),
            pltpu.VMEM((2, PIECE, BLOCK), jnp.bfloat16),
            pltpu.VMEM((2, PIECE, BLOCK), jnp.bfloat16),
            pltpu.VMEM((2, PIECE // 2, BLOCK), jnp.bfloat16),
            pltpu.VMEM((2, PIECE, BLOCK), jnp.bfloat16),
            pltpu.VMEM((2, PIECE, BLOCK), jnp.bfloat16),
            pltpu.VMEM((NX * NZ, OWN, BLOCK), jnp.float32),
            pltpu.VMEM((NX * NZ - 1, OWN, BLOCK), jnp.float32),
            pltpu.VMEM((ROWS, KVL), jnp.float32),
            pltpu.VMEM((NT - 1, PART, KVL), jnp.float32),
            pltpu.VMEM((NT, 1, KVL), jnp.float32),
            pltpu.VMEM((NX * NZ, 1, KVL), jnp.float32),
            pltpu.VMEM((NY, 1, KVL), jnp.float32),
            dma((5,)),
            dma((NX - 1,)),
            dma((NX - 1,)),
            dma((NX - 1,)),
            dma((NX - 1,)),
            dma((NX - 1, chunks)),
            dma((NX - 1, chunks)),
            dma((8, chunks)),
            dma((8, chunks)),
            dma((NX * NZ - 1, len(BATCHES))),
            dma((NX * NZ - 1, len(BATCHES))),
            dma((NT - 1,)),
            dma((NT - 1,)),
            dma((NT - 1,)),
            dma((NT - 1,)),
            dma((gains,)),
            dma((gains,)),
        ],
        compiler_params=pltpu.CompilerParams(collective_id=0, has_side_effects=True),
        name="norm_up_backward",
    )(latent_raw, norm_gain.reshape(1, KVL), up_weight, grad_kv)
    latent_grad, gain_grad, weight_grad = pl.pallas_call(
        store, out_shape=shapes, in_specs=[vmem] * 3, out_specs=(vmem,) * 3, name="store",
    )(*results)
    return latent_grad, gain_grad.reshape(KVL), weight_grad


def solution(mesh):
    split = Mesh(mesh.devices.reshape(NX, NY, NZ, NH, NC), AXES)
    in_specs = (P(DP, None), P(), P(None, TENSOR), P(DP, TENSOR))
    out_specs = (P(DP, None), P(), P(DP, TENSOR))
    return jax.shard_map(
        per_device, mesh=split, in_specs=in_specs, out_specs=out_specs, check_vma=False
    )
```

```python
import functools

import jax
import jax.numpy as jnp
from jax import lax
from jax.experimental import pallas as pl
from jax.experimental.pallas import tpu as pltpu
from jax.sharding import Mesh
from jax.sharding import PartitionSpec as P

X, Y, Z, H, C = AXES = ("dp_0", "dp_1", "dp_2", "tensor_0", "tensor_1")
DP = (X, Y, Z)
TENSOR = (H, C)
NX, NY, NZ, NH, NC = 4, 8, 4, 3, 2
NT = NH * NC
SIZE = dict(zip(AXES, (NX, NY, NZ, NH, NC)))
MESH = pl.DeviceIdType.MESH

KVL = 512
COLS = 4096
ROWS = 192
BLOCK = COLS // NX
PART = ROWS // NT
OWN = KVL // (NX * NY * NZ)
STRIP = OWN * NZ
epsilon = 1e-06

CHUNKS = ((0, 256), (256, 256), (512, 256), (768, 128), (896, 128))
BATCHES = ((0, 512), (512, 384), (896, 128))
BATCH_AFTER = {1: 0, 3: 1, 4: 2}
SCHEDULE = (
    ("W", 0), ("W", 1), ("R", 0), ("W", 2), ("G", 1), ("R", 1), ("S", 0), ("W", 3), ("W", 4),
    ("R", 2), ("S", 1), ("R", 3), ("G", 2), ("R", 4), ("S", 2), ("S", 3), ("S", 4), ("G", 3), ("L", 0),
)
HALF = ROWS // NC
PIECE = OWN * NZ * NX

X_OFFSETS = (1, 3, 2)
Y_OFFSETS = (1, 7, 2, 6, 3, 5, 4)
XZ_OFFSETS = tuple((i, j) for i in range(NX) for j in range(NZ) if (i, j) != (0, 0))
T_OFFSETS = tuple((i, j) for i in range(NH) for j in range(NC) if (i, j) != (0, 0))


def shifted(axis, offset):
    return lax.rem(lax.axis_index(axis) + (offset % SIZE[axis]), SIZE[axis])


def at(**offsets):
    return {axis: shifted(axis, offset) for axis, offset in offsets.items() if offset % SIZE[axis]}


def normalize(latent):
    full = latent.astype(jnp.float32)
    inverse = lax.rsqrt(jnp.mean(full * full, axis=-1, keepdims=True) + epsilon)
    return full * inverse, inverse


def kernel(
    factor,
    latent_hbm, gain_hbm, up_hbm, grad_hbm,
    latent_out, gain_out, weight_out,
    latent, gain, up, grad, normed, tokens, full, wsend, direct, far, farther, rsend, relayed,
    esend, ebuf, tsend, tpair, tsum, tbuf, g1, g2, g3,
    local_sem, ns, nr, fs, fr, xs, xr, ys, yr, es, er, ps, pr, ts, tr, ls, lr, gs, gr,
):
    x, y, z = (lax.axis_index(a) for a in DP)
    core = lax.axis_index(C)
    t = lax.axis_index(H) * NC + core
    sends = []

    def send(src, dst, send_sem, recv_sem, device):
        copy = pltpu.make_async_remote_copy(
            src_ref=src, dst_ref=dst, send_sem=send_sem, recv_sem=recv_sem,
            device_id=device, device_id_type=MESH,
        )
        copy.start()
        sends.append(copy)
        return copy

    loads = [
        pltpu.make_async_copy(latent_hbm, latent, local_sem.at[0]),
        pltpu.make_async_copy(gain_hbm, gain, local_sem.at[1]),
        pltpu.make_async_copy(grad_hbm, grad, local_sem.at[2]),
        pltpu.make_async_copy(
            grad_hbm.at[:, pl.ds(pl.multiple_of(x * BLOCK, BLOCK), BLOCK)],
            tokens.at[pl.ds(0, ROWS), :], local_sem.at[3],
        ),
        pltpu.make_async_copy(up_hbm, up, local_sem.at[4]),
    ]
    for load in loads:
        load.start()

    barrier = pltpu.get_barrier_semaphore()
    devices = [at(**{H: i, C: j}) for i, j in T_OFFSETS]
    devices += [at(**{X: i, Z: j}) for i, j in XZ_OFFSETS]
    devices += [at(**{Y: i}) for i in Y_OFFSETS]
    for device in devices:
        pl.semaphore_signal(barrier, inc=1, device_id=device, device_id_type=MESH)

    loads[0].wait()
    loads[1].wait()
    scaled, _ = normalize(latent[...])
    normed[pl.ds(0, ROWS), :] = (scaled * gain[...]).astype(jnp.bfloat16)
    pl.semaphore_wait(barrier, len(devices))

    def half(i):
        return pl.ds(pl.multiple_of(ROWS * i + HALF * core, HALF), HALF)

    halves = []
    for n, i in enumerate(X_OFFSETS):
        halves.append(send(
            normed.at[half(0), :], normed.at[half(i), :], ns.at[n], nr.at[n], at(**{X: i})
        ))
    loads[2].wait()
    xsends = {}
    for k, (start, width) in enumerate(CHUNKS):
        for n, i in enumerate(X_OFFSETS):
            column = pl.multiple_of(shifted(X, i) * BLOCK + start, 128)
            xsends[k, i] = send(
                grad.at[:, pl.ds(column, width)],
                tokens.at[pl.ds(ROWS * i, ROWS), pl.ds(start, width)],
                xs.at[n, k], xr.at[n, k], at(**{X: i}),
            )

    loads[4].wait()
    tsend[...] = lax.dot_general(
        grad[...], up[...], (((1,), (1,)), ((), ())), preferred_element_type=jnp.float32
    ).reshape(NH, NC, PART, KVL)
    sibling = at(**{C: 1})
    tpaired = send(
        tsend.at[:, lax.rem(core + 1, NC)], tpair, ps.at[0], pr.at[0], sibling
    )
    loads[3].wait()
    forwards = []
    for n, i in enumerate(X_OFFSETS):
        halves[n].wait_recv()
        forwards.append(send(
            normed.at[half(i), :], normed.at[half(i), :], fs.at[n], fr.at[n], sibling
        ))
    tpaired.wait_recv()
    for h in range(NH):
        tsum[h] = tsend[h, core] + tpair[h]
    tsends = [
        send(tsum.at[shifted(H, i)], tbuf.at[i - 1], ts.at[i - 1], tr.at[i - 1], at(**{H: i}))
        for i in range(1, NH)
    ]

    def rows_of(other, p):
        return pl.ds(pl.multiple_of(128 * p + STRIP * other, STRIP), STRIP)

    def weight_chunk(k):
        start, width = CHUNKS[k]
        columns = slice(start, start + width)
        if k == 0:
            for copy in forwards:
                copy.wait_recv()
        for i in X_OFFSETS:
            xsends[k, i].wait_recv()
        full[:, columns] = lax.dot_general(
            normed[...], tokens[:, columns], (((0,), (0,)), ((), ())),
            preferred_element_type=jnp.float32,
        )
        for slot, offset in enumerate((3, -3, 4, 1, -1)):
            for p in range(NX):
                wsend[slot, STRIP * p : STRIP * (p + 1), columns] = full[
                    rows_of(shifted(Y, offset), p), columns
                ].astype(jnp.bfloat16)
        window = pl.ds(start, width)
        into_relay, into_total = [], []
        for side, sign in enumerate((1, -1)):
            into_relay.append(send(
                wsend.at[side, :, window], far.at[side, :, window],
                ys.at[side, k], yr.at[side, k], at(**{Y: sign}),
            ))
        for side, sign in enumerate((1, -1)):
            into_relay.append(send(
                wsend.at[2, pl.ds(PIECE // 2 * side, PIECE // 2), window],
                farther.at[side, :, window],
                ys.at[2 + side, k], yr.at[2 + side, k], at(**{Y: 2 * sign}),
            ))
        for side, sign in enumerate((1, -1)):
            into_total.append(send(
                wsend.at[3 + side, :, window], direct.at[side, :, window],
                ys.at[4 + side, k], yr.at[4 + side, k], at(**{Y: sign}),
            ))
        return into_relay, into_total

    def relay_chunk(k, into_relay):
        start, width = CHUNKS[k]
        columns = slice(start, start + width)
        for copy in into_relay:
            copy.wait_recv()
        copies = []
        for side, sign in enumerate((1, -1)):
            for p in range(NX):
                part = slice(STRIP * p, STRIP * (p + 1))
                total = full[rows_of(shifted(Y, 2 * sign), p), columns]
                total = total + far[side, part, columns].astype(jnp.float32)
                if p // 2 == side:
                    start_row = STRIP * (p - 2 * side)
                    total = total + farther[
                        side, start_row : start_row + STRIP, columns
                    ].astype(jnp.float32)
                rsend[side, part, columns] = total.astype(jnp.bfloat16)
            window = pl.ds(start, width)
            copies.append(send(
                rsend.at[side, :, window], relayed.at[side, :, window],
                ys.at[6 + side, k], yr.at[6 + side, k], at(**{Y: 2 * sign}),
            ))
        return copies

    def sum_chunk(k, copies):
        start, width = CHUNKS[k]
        columns = slice(start, start + width)
        for copy in copies:
            copy.wait_recv()
        for p in range(NX):
            part = slice(STRIP * p, STRIP * (p + 1))
            total = full[rows_of(y, p), columns]
            for source in (direct, relayed):
                for side in range(2):
                    total = total + source[side, part, columns].astype(jnp.float32)
            for q in range(NZ):
                esend[NZ * p + q, :, columns] = total[OWN * q : OWN * (q + 1)]

    def exchange(b):
        start, width = BATCHES[b]
        copies = []
        for n, (i, j) in enumerate(XZ_OFFSETS):
            copies.append(send(
                esend.at[shifted(X, i) * NZ + shifted(Z, j), :, pl.ds(start, width)],
                ebuf.at[n, :, pl.ds(start, width)],
                es.at[n, b], er.at[n, b], at(**{X: i, Z: j}),
            ))
        return copies

    def latent_step():
        for copy in tsends:
            copy.wait_recv()
        own = pl.ds(pl.multiple_of(t * PART, PART), PART)
        grad_norm = tsum[lax.axis_index(H)]
        for n in range(NH - 1):
            grad_norm = grad_norm + tbuf[n]
        scaled, inverse = normalize(latent[own, :])
        g1[t] = jnp.sum(grad_norm * scaled, axis=0, keepdims=True)
        upstream = grad_norm * gain[...]
        centred = upstream - scaled * jnp.mean(upstream * scaled, axis=-1, keepdims=True)
        latent_out[own, :] = (inverse * centred).astype(jnp.bfloat16)
        copies = []
        for n, (i, j) in enumerate(T_OFFSETS):
            copies.append(send(
                g1.at[t], g1.at[t], gs.at[n], gr.at[n], at(**{H: i, C: j})
            ))
        lcopies = [
            send(
                latent_out.at[own, :], latent_out.at[own, :], ls.at[n], lr.at[n], device
            )
            for n, device in enumerate((at(**{H: 1}), at(**{H: 2}), sibling))
        ]
        return copies, lcopies

    def forward_step(lcopies):
        copies = lcopies[2:]
        for n, i in enumerate((1, 2)):
            lcopies[n].wait_recv()
            part = shifted(H, -i) * NC + core
            rows = pl.ds(pl.multiple_of(part * PART, PART), PART)
            copies.append(send(
                latent_out.at[rows, :], latent_out.at[rows, :], ls.at[3 + n], lr.at[3 + n], sibling
            ))
        return copies

    def gain_step(copies, source, target, slot, offsets, first):
        for copy in copies:
            copy.wait_recv()
        total = source[0]
        for n in range(1, source.shape[0]):
            total = total + source[n]
        target[slot] = total
        copies = []
        for n, offset in enumerate(offsets):
            copies.append(send(
                target.at[slot], target.at[slot], gs.at[first + n], gr.at[first + n], at(**offset)
            ))
        return copies

    into_relay, into_total, received = {}, {}, []
    gcopies = lcopies = None
    for kind, k in SCHEDULE:
        if kind == "W":
            into_relay[k], into_total[k] = weight_chunk(k)
        elif kind == "R":
            into_total[k] += relay_chunk(k, into_relay[k])
        elif kind == "S":
            sum_chunk(k, into_total[k])
            if k in BATCH_AFTER:
                received += exchange(BATCH_AFTER[k])
        elif kind == "G" and k == 1:
            gcopies, lcopies = latent_step()
        elif kind == "L":
            lcopies = forward_step(lcopies)
        elif kind == "G" and k == 2:
            gcopies = gain_step(
                gcopies, g1, g2, x * NZ + z, [{X: i, Z: j} for i, j in XZ_OFFSETS], NT - 1
            )
        else:
            gcopies = gain_step(
                gcopies, g2, g3, y, [{Y: i} for i in Y_OFFSETS], NT - 1 + NX * NZ - 1
            )
    for copy in lcopies:
        copy.wait_recv()
    for copy in received:
        copy.wait_recv()
    for i in range(NX):
        total = None
        for j in range(NZ):
            if (i, j) == (0, 0):
                term = esend[x * NZ + z]
            else:
                term = ebuf[XZ_OFFSETS.index((i, j))]
            total = term if total is None else total + term
        column = pl.multiple_of(shifted(X, -i) * BLOCK, BLOCK)
        weight_out[:, pl.ds(column, BLOCK)] = total * factor
    for copy in gcopies:
        copy.wait_recv()
    total = g3[0]
    for n in range(1, NY):
        total = total + g3[n]
    gain_out[...] = total * factor
    for copy in sends:
        copy.wait_send()


def store(*refs):
    for source, target in zip(refs[:3], refs[3:]):
        target[...] = source[...]


def per_device(latent_raw, norm_gain, up_weight, grad_kv):
    factor = float(latent_raw.shape[0] * NX * NY * NZ) ** (-0.5)
    vmem = pl.BlockSpec(memory_space=pltpu.VMEM)
    hbm = pl.BlockSpec(memory_space=pl.ANY)
    dma = pltpu.SemaphoreType.DMA
    gains = NT - 1 + NX * NZ - 1 + NY - 1
    chunks = len(CHUNKS)
    shapes = (
        jax.ShapeDtypeStruct((ROWS, KVL), jnp.bfloat16),
        jax.ShapeDtypeStruct((1, KVL), jnp.float32),
        jax.ShapeDtypeStruct((OWN, COLS), jnp.float32),
    )
    results = pl.pallas_call(
        functools.partial(kernel, factor),
        out_shape=shapes,
        in_specs=[hbm, hbm, hbm, hbm],
        out_specs=(vmem, vmem, vmem),
        scratch_shapes=[
            pltpu.VMEM((ROWS, KVL), jnp.bfloat16),
            pltpu.VMEM((1, KVL), jnp.float32),
            pltpu.VMEM((KVL, COLS), jnp.bfloat16),
            pltpu.VMEM((ROWS, COLS), jnp.bfloat16),
            pltpu.VMEM((NX * ROWS, KVL), jnp.bfloat16),
            pltpu.VMEM((NX * ROWS, BLOCK), jnp.bfloat16),
            pltpu.VMEM((KVL, BLOCK), jnp.float32),
            pltpu.VMEM((5, PIECE, BLOCK), jnp.bfloat16),
            pltpu.VMEM((2, PIECE, BLOCK), jnp.bfloat16),
            pltpu.VMEM((2, PIECE, BLOCK), jnp.bfloat16),
            pltpu.VMEM((2, PIECE // 2, BLOCK), jnp.bfloat16),
            pltpu.VMEM((2, PIECE, BLOCK), jnp.bfloat16),
            pltpu.VMEM((2, PIECE, BLOCK), jnp.bfloat16),
            pltpu.VMEM((NX * NZ, OWN, BLOCK), jnp.float32),
            pltpu.VMEM((NX * NZ - 1, OWN, BLOCK), jnp.float32),
            pltpu.VMEM((NH, NC, PART, KVL), jnp.float32),
            pltpu.VMEM((NH, PART, KVL), jnp.float32),
            pltpu.VMEM((NH, PART, KVL), jnp.float32),
            pltpu.VMEM((NH - 1, PART, KVL), jnp.float32),
            pltpu.VMEM((NT, 1, KVL), jnp.float32),
            pltpu.VMEM((NX * NZ, 1, KVL), jnp.float32),
            pltpu.VMEM((NY, 1, KVL), jnp.float32),
            dma((5,)),
            dma((NX - 1,)),
            dma((NX - 1,)),
            dma((NX - 1,)),
            dma((NX - 1,)),
            dma((NX - 1, chunks)),
            dma((NX - 1, chunks)),
            dma((8, chunks)),
            dma((8, chunks)),
            dma((NX * NZ - 1, len(BATCHES))),
            dma((NX * NZ - 1, len(BATCHES))),
            dma((1,)),
            dma((1,)),
            dma((NH - 1,)),
            dma((NH - 1,)),
            dma((NT - 1,)),
            dma((NT - 1,)),
            dma((gains,)),
            dma((gains,)),
        ],
        compiler_params=pltpu.CompilerParams(collective_id=0, has_side_effects=True),
        name="norm_up_backward",
    )(latent_raw, norm_gain.reshape(1, KVL), up_weight, grad_kv)
    latent_grad, gain_grad, weight_grad = pl.pallas_call(
        store, out_shape=shapes, in_specs=[vmem] * 3, out_specs=(vmem,) * 3, name="store",
    )(*results)
    return latent_grad, gain_grad.reshape(KVL), weight_grad


def solution(mesh):
    split = Mesh(mesh.devices.reshape(NX, NY, NZ, NH, NC), AXES)
    in_specs = (P(DP, None), P(), P(None, TENSOR), P(DP, TENSOR))
    out_specs = (P(DP, None), P(), P(DP, TENSOR))
    return jax.shard_map(
        per_device, mesh=split, in_specs=in_specs, out_specs=out_specs, check_vma=False
    )
```
